32 devices in a mesh: dp: 16 (over z, y, x), mp: 2 (over core).
Axes of the slice: x: 2, y: 2, z: 4, core: 2. Of those that a mesh axis runs over, the one named last changes fastest.
Arguments:
- hidden: bfloat16 [240, 128, 2048], P('dp', None, 'mp'), may hold values from -6 to 6
- attn_out: bfloat16 [240, 128, 2048], P('dp', None, 'mp'), may hold values from -6 to 6
- out_proj: bfloat16 [2048, 2048], P(None, 'mp'), may hold values from -0.125 to 0.125
- norm_gain: float32 [2048], P('mp'), may hold values from 0.1 to 1.9
- reward_proj: float32 [2048, 8], P('mp'), may hold values from -0.125 to 0.125
- block_seq: int32 [240], replicated, may hold values from -1 to 95, as said below
- block_dest: int32 [240], replicated, may hold values from -1 to 159, as said below
- lengths: int32 [96], replicated, may hold values from 1 to 512, as said below
Outputs:
- token_rewards: float32 [160, 8, 128], P('dp')
- advantages: float32 [96], P('dp')
The draws below stay inside these ranges and needn't reach their ends.
Inputs may be any that keep to these rules, and one draw needn't show every extreme that they name: `block_seq`: used slots of each index of dp come first in its 15 slots, the rest hold -1; each index of dp holds 1 to 15 used slots and some index holds exactly 15. Read over used slots in slot order, response numbers never fall, every response appears, and each has 1 to 4 blocks. `block_dest`: exactly the used slots (those of block_seq that are not -1) hold a destination; every owned slot of every owner is named exactly once, so each owner receives exactly 10 blocks; at most 1 block go from one index of dp to one owner, and that many in some pair. `lengths`: A response of n blocks has more than 128 * (n - 1) and at most 128 * n tokens.
All inputs are finite; a program needn't handle non-finite values.
Results may differ from the reference program's by a relative error of at most 0.0029.
Values may be sent and summed in bfloat16 or wider, within the bound.
A program may use at most 64 MiB of HBM per device.

```python
import jax
import jax.numpy as jnp
from jax import lax

D = 2048
HEADS_R = 8
BLK = 128
MOSTB = 4
OWN_CAP = 10
SLOTS_IN = 15
SEQS = 96
BLOCKS_IN = 240
N_DP = 16


def plan_tables(key):
    base = jax.random.fold_in(key, 4242)
    key_busy, key_cells, key_seqs, key_turn, key_owner, key_length = jax.random.split(base, 6)
    key_longest = jax.random.fold_in(base, 7)
    device_count = BLOCKS_IN // SLOTS_IN
    block_total = OWN_CAP * device_count
    busiest = jax.random.randint(key_busy, (), 0, device_count)
    room_left = SLOTS_IN - 1
    extra_blocks = block_total - (device_count - 1) - SLOTS_IN
    cell_order = jax.random.permutation(key_cells, (device_count - 1) * room_left)
    chosen = (cell_order < extra_blocks).astype(jnp.int32).reshape(device_count - 1, room_left).sum(axis=1)
    positions = jnp.arange(device_count, dtype=jnp.int32)
    shifted = jnp.clip(positions - (positions > busiest).astype(jnp.int32), 0, device_count - 2)
    counts = jnp.where(positions == busiest, SLOTS_IN, 1 + chosen[shifted]).astype(jnp.int32)
    starts = jnp.cumsum(counts) - counts
    slot_pos = jnp.arange(SLOTS_IN, dtype=jnp.int32)
    is_used = (slot_pos[None, :] < counts[:, None]).reshape(-1)
    global_pos = (starts[:, None] + slot_pos[None, :]).reshape(-1)
    global_pos = jnp.where(is_used, global_pos, 0)
    seq_extra = block_total - SEQS
    cell_total = SEQS * (MOSTB - 1)
    longest = jax.random.randint(key_longest, (), 0, SEQS)
    seq_cells = jax.random.permutation(key_seqs, cell_total).astype(jnp.int32)
    cell_index = jnp.arange(cell_total, dtype=jnp.int32)
    cell_row = cell_index // (MOSTB - 1)
    sort_keys = jnp.where(cell_row == longest, -1 - cell_index % (MOSTB - 1), seq_cells)
    cell_rank = jnp.argsort(jnp.argsort(sort_keys, stable=True), stable=True).astype(jnp.int32)
    seq_blocks = 1 + (cell_rank < seq_extra).astype(jnp.int32).reshape(SEQS, MOSTB - 1).sum(axis=1)
    seq_starts = jnp.cumsum(seq_blocks) - seq_blocks
    seq_of = (seq_starts[None, :] <= global_pos[:, None]).astype(jnp.int32).sum(axis=1) - 1
    block_seq = jnp.where(is_used, seq_of, -1)
    rotation = jax.random.randint(key_turn, (), 0, device_count)
    owner_order = jax.random.permutation(key_owner, device_count)
    owner_rank = owner_order[(global_pos + rotation) % device_count]
    destination = jnp.where(is_used, owner_rank * OWN_CAP + global_pos // device_count, -1)
    tail_tokens = jax.random.randint(key_length, (SEQS,), 1, BLK + 1)
    seq_ids = jnp.arange(SEQS, dtype=jnp.int32)
    tail_tokens = jnp.where(seq_ids == longest, BLK, tail_tokens)
    lengths = BLK * (seq_blocks - 1) + tail_tokens
    return (block_seq.astype(jnp.int32), destination.astype(jnp.int32), lengths.astype(jnp.int32))


def draw_block_seq(key, part):
    return plan_tables(key)[0]


def draw_block_dest(key, part):
    return plan_tables(key)[1]


def draw_lengths(key, part):
    return plan_tables(key)[2]


def shard_levels(key, dims, shards, least, largest):
    loudness, own = 1.0, jax.random.fold_in(key, 6)
    for axis_at, shards_of in shards:
        heights = jnp.exp(jax.random.uniform(jax.random.fold_in(own, axis_at), (shards_of,), jnp.float32, least / len(shards), largest / len(shards)))
        loudness = loudness * jnp.repeat(heights, dims[axis_at] // shards_of).reshape([-1 if axis == axis_at else 1 for axis in range(len(dims))])
    return loudness


def centred(rng, dims, scale, reach, pieces=(), kind=jnp.bfloat16):
    loudness = shard_levels(rng, dims, pieces, -0.22, 0.18) if pieces else 1.0
    entries = jax.random.normal(rng, dims, jnp.float32) * scale * loudness
    return jnp.minimum(jnp.maximum(entries, -reach), reach).astype(kind)


def setup_inputs(seed: int = 0) -> dict:
    arg_keys = jax.random.split(jax.random.key(seed), 9)
    return {
        "hidden": centred(arg_keys[0], (BLOCKS_IN, BLK, D), 1.0, 6.0, ((0, 16), (2, 2))),
        "attn_out": centred(arg_keys[1], (BLOCKS_IN, BLK, D), 1.0, 6.0, ((0, 16), (2, 2))),
        "out_proj": centred(arg_keys[2], (D, D), D ** -0.5, 0.125, ((1, 2),)),
        "norm_gain": jnp.clip(1.0 + 0.18 * jax.random.normal(arg_keys[3], (D,), jnp.float32), 0.1, 1.9),
        "reward_proj": centred(arg_keys[4], (D, HEADS_R), D ** -0.5, 0.125, ((0, 2),), jnp.float32),
        "block_seq": draw_block_seq(jax.random.fold_in(arg_keys[8], 71), 0),
        "block_dest": draw_block_dest(jax.random.fold_in(arg_keys[8], 71), 0),
        "lengths": draw_lengths(jax.random.fold_in(arg_keys[8], 71), 0),
    }


norm_epsilon = 1e-05
stat_epsilon = 1e-06

def reference(hidden, attn_out, out_proj, norm_gain, reward_proj, block_seq, block_dest, lengths):
    slot_count = block_seq.shape[0]
    owned_count = OWN_CAP * N_DP
    slot_index = jnp.arange(slot_count, dtype=jnp.int32)
    is_used = block_dest >= 0
    target = jnp.where(is_used, block_dest, owned_count).astype(jnp.int32)
    source = jnp.zeros((owned_count,), jnp.int32).at[target].set(slot_index, mode='drop')
    seq_safe = jnp.where(is_used, block_seq, 0).astype(jnp.int32)
    used_int = is_used.astype(jnp.int32)
    per_seq = jnp.zeros((SEQS,), jnp.int32).at[seq_safe].add(used_int)
    seq_starts = jnp.cumsum(per_seq) - per_seq
    global_pos = jnp.cumsum(used_int) - 1
    seq_rank = global_pos - seq_starts[seq_safe]
    valid_tokens = jnp.minimum(BLK, lengths[seq_safe] - BLK * seq_rank)
    src_seq = seq_safe[source]
    src_valid = valid_tokens[source]

    def one_block(slot):
        projected = jnp.dot(attn_out[slot], out_proj, preferred_element_type=jnp.float32)
        stored = (hidden[slot].astype(jnp.float32) + projected).astype(jnp.bfloat16)
        stored = lax.optimization_barrier(stored)
        values = stored.astype(jnp.float32)
        mean_sq = lax.optimization_barrier(jnp.mean(values * values, axis=1, keepdims=True))
        normed = values * lax.rsqrt(mean_sq + norm_epsilon) * norm_gain[None, :]
        return jnp.dot(normed, reward_proj, precision=lax.Precision.HIGHEST)
    rewards = lax.map(one_block, source)
    live = jnp.arange(BLK, dtype=jnp.int32)[None, :] < src_valid[:, None]
    rewards = jnp.where(live[:, :, None], rewards, jnp.float32(0.0))
    token_rewards = jnp.transpose(rewards, (0, 2, 1))
    block_sums = lax.optimization_barrier(jnp.sum(token_rewards, axis=2))
    seq_totals = jnp.zeros((SEQS, HEADS_R), jnp.float32).at[src_seq].add(block_sums)
    scores = seq_totals / lengths[:, None].astype(jnp.float32)
    worst_case = lax.optimization_barrier(jnp.min(scores, axis=1))
    head_mean = lax.optimization_barrier(jnp.mean(scores, axis=1))
    spread = lax.optimization_barrier(jnp.mean((scores - head_mean[:, None]) ** 2, axis=1))
    penalty_scale = jnp.mean(spread) + stat_epsilon
    conservative = worst_case - spread / penalty_scale
    centre = jnp.mean(conservative)
    variance = jnp.mean((conservative - centre) ** 2)
    advantages = (conservative - centre) / jnp.sqrt(variance + stat_epsilon)
    return (token_rewards, advantages)
```

```python
import functools

import jax
import jax.numpy as jnp
from jax import lax
from jax.experimental import pallas as pl
from jax.experimental.pallas import tpu as pltpu
from jax.sharding import PartitionSpec as P

OWN_CAP = 10

norm_epsilon = 1e-05
stat_epsilon = 1e-06
MESH = pl.DeviceIdType.MESH
LANES = 128


def split_slots(slots):
    third = max(1, slots // 3)
    first = ((0, third), (third, slots)) if slots > third else ((0, slots),)
    cuts = [*range(0, slots - third + 1, third), slots]
    second = tuple(zip(cuts[:-1], cuts[1:]))
    return first, second, second


def partner(index, k, n):
    if n & (n - 1):
        return lax.rem(index + k, n)
    out = index
    bit = 1
    while bit < n:
        if k & bit:
            out = out + bit - 2 * bit * lax.rem(lax.div(index, bit), 2)
        bit *= 2
    return out


def kernel(
    n_dp, n_mp, slots, block_len, seq_count, groups,
    hidden_hbm, attn_hbm, w_hbm, gain_hbm, reward_hbm, seq_hbm, dest_hbm, len_hbm,
    rewards_out, adv_out,
    attn, w, hidden, acc, resid, heads_w, part, live, rewards, seq_acc, send_buf,
    recv_sum, recv_rew, adv_buf,
    send_idx, gain_ref, reward_ref, seq_s, dest_s, len_s, seq_v, dest_v, len_v, small_sem,
    w_sem, own_sem, hid_sem, attn_send, attn_recv, part_send, part_recv,
    sum_send, sum_recv, rew_send, rew_recv,
):
    dp = lax.axis_index("dp")
    mp = lax.axis_index("mp")
    first_ranges, second_ranges, head_ranges = groups
    k_local = attn_hbm.shape[1]
    n_local = w_hbm.shape[1]
    model_width = w_hbm.shape[0]
    chunk = min(256, n_local)
    n_chunks = n_local // chunk
    head_count = reward_ref.shape[0]
    h = head_count
    base = dp * slots

    barrier = pltpu.get_barrier_semaphore()
    for off in range(1, n_mp):
        pl.semaphore_signal(barrier, inc=1, device_id=(dp, lax.rem(mp + off, n_mp)), device_id_type=MESH)
    for k in range(n_dp - 1, 0, -1):
        pl.semaphore_signal(barrier, inc=1, device_id=(partner(dp, k, n_dp), mp), device_id_type=MESH)

    def block_rows(blocks):
        return slice(blocks[0] * block_len, blocks[1] * block_len)

    k_half = k_local // 2

    def w_copy(off, half):
        start = pl.multiple_of(lax.rem(mp + off, n_mp) * k_local + half * k_half, k_half)
        return pltpu.make_async_copy(
            w_hbm.at[pl.ds(start, k_half)], w.at[off, half * k_half : (half + 1) * k_half], w_sem.at[off, half]
        )

    def lead_copy(half):
        rows = block_rows(first_ranges[0])
        cols = slice(half * k_half, (half + 1) * k_half)
        return pltpu.make_async_copy(attn_hbm.at[rows, cols], attn.at[0, rows, cols], own_sem.at[half])

    def own_copy(i):
        rows = block_rows(first_ranges[i])
        return pltpu.make_async_copy(attn_hbm.at[rows], attn.at[0, rows], own_sem.at[i + 1])

    def other_w(action):
        for off in range(1, n_mp):
            for half in range(2):
                getattr(w_copy(off, half), action)()

    def hid_copy(i):
        rows = block_rows(second_ranges[i])
        return pltpu.make_async_copy(hidden_hbm.at[rows], hidden.at[rows], hid_sem.at[i])

    def attn_copy(off, i):
        rows = block_rows(second_ranges[i])
        return pltpu.make_async_remote_copy(
            src_ref=attn_hbm.at[rows],
            dst_ref=attn.at[n_mp - off, rows],
            send_sem=attn_send.at[off - 1, i],
            recv_sem=attn_recv.at[off - 1, i],
            device_id=(dp, lax.rem(mp + off, n_mp)),
            device_id_type=MESH,
        )

    def part_copy(off, i):
        rows = block_rows(head_ranges[i])
        return pltpu.make_async_remote_copy(
            src_ref=part.at[0, :, rows],
            dst_ref=part.at[n_mp - off, :, rows],
            send_sem=part_send.at[off - 1, i],
            recv_sem=part_recv.at[off - 1, i],
            device_id=(dp, lax.rem(mp + off, n_mp)),
            device_id_type=MESH,
        )

    def sum_copy(k):
        return pltpu.make_async_remote_copy(
            src_ref=seq_acc,
            dst_ref=recv_sum.at[dp],
            send_sem=sum_send,
            recv_sem=sum_recv,
            device_id=(partner(dp, k, n_dp), mp),
            device_id_type=MESH,
        )

    def rew_copy(k):
        peer = partner(dp, k, n_dp)
        return pltpu.make_async_remote_copy(
            src_ref=send_buf.at[peer],
            dst_ref=recv_rew.at[dp],
            send_sem=rew_send,
            recv_sem=rew_recv,
            device_id=(peer, mp),
            device_id_type=MESH,
        )

    def wait_all(ref, sem):
        others = ref.at[0 : n_dp - 1]
        pltpu.make_async_copy(others, others, sem).wait()

    w_copy(0, 0).start()
    lead_copy(0).start()
    small = [
        pltpu.make_async_copy(src, dst, small_sem.at[i])
        for i, (src, dst) in enumerate(
            (
                (gain_hbm, gain_ref),
                (reward_hbm, reward_ref),
                (seq_hbm, seq_s),
                (dest_hbm, dest_s),
                (len_hbm, len_s),
                (seq_hbm, seq_v),
                (dest_hbm, dest_v),
                (len_hbm, len_v),
            )
        )
    ]
    for copy in small:
        copy.start()
    with jax.named_scope("smallw"):
        small[0].wait()
        small[1].wait()
    weighted = reward_ref[...] * gain_ref[...].reshape(1, n_local)
    high = weighted.astype(jnp.bfloat16)
    rest = weighted - high.astype(jnp.float32)
    middle = rest.astype(jnp.bfloat16)
    low = (rest - middle.astype(jnp.float32)).astype(jnp.bfloat16)
    heads_w[...] = jnp.concatenate([high, middle, low, jnp.zeros_like(low)], axis=0)
    seq_acc[...] = jnp.zeros_like(seq_acc)

    def first_half(i):
        rows = block_rows(first_ranges[i])
        for c in range(n_chunks):
            cols = slice(c * chunk, (c + 1) * chunk)
            acc[rows, cols] = jnp.dot(attn[0, rows, :], w[0, :, cols], preferred_element_type=jnp.float32)

    def lead(half):
        rows = block_rows(first_ranges[0])
        depth = slice(half * k_half, (half + 1) * k_half)
        for c in range(n_chunks):
            cols = slice(c * chunk, (c + 1) * chunk)
            product = jnp.dot(attn[0, rows, depth], w[0, depth, cols], preferred_element_type=jnp.float32)
            acc[rows, cols] = acc[rows, cols] + product if half else product

    def send_attn(i):
        if i < len(second_ranges):
            for off in range(1, n_mp):
                attn_copy(off, i).start()

    w_copy(0, 1).start()
    lead_copy(1).start()
    with jax.named_scope("lead0"):
        w_copy(0, 0).wait()
        lead_copy(0).wait()
    for i in range(1, len(first_ranges)):
        own_copy(i).start()
    lead(0)
    with jax.named_scope("barr"):
        pl.semaphore_wait(barrier, n_mp - 1 + n_dp - 1)
    send_attn(0)
    with jax.named_scope("lead1"):
        w_copy(0, 1).wait()
        lead_copy(1).wait()
    lead(1)
    send_attn(1)
    other_w("start")
    for i in range(1, len(first_ranges)):
        with jax.named_scope("ownw"):
            own_copy(i).wait()
        if i == 1:
            for j in range(len(second_ranges)):
                hid_copy(j).start()
        first_half(i)
    for i in range(2, len(second_ranges)):
        send_attn(i)

    seq_lane = lax.broadcasted_iota(jnp.int32, (head_count, seq_acc.shape[1]), 1)

    def second_half(i):
        rows = block_rows(second_ranges[i])
        for c in range(n_chunks):
            cols = slice(c * chunk, (c + 1) * chunk)
            total = acc[rows, cols]
            for off in range(1, n_mp):
                total = total + jnp.dot(attn[off, rows, :], w[off, :, cols], preferred_element_type=jnp.float32)
            resid[rows, cols] = (hidden[rows, cols].astype(jnp.float32) + total).astype(jnp.bfloat16)

    def head_sums(i):
        rows = block_rows(head_ranges[i])
        count = rows.stop - rows.start
        out = lax.dot_general(
            heads_w[...], resid[rows, :], (((1,), (1,)), ((), ())), preferred_element_type=jnp.float32
        )
        part[0, 0:h, rows] = out[0:h] + out[h : 2 * h] + out[2 * h : 3 * h]
        squares = jnp.zeros((count, LANES), jnp.float32)
        for c in range(n_local // LANES):
            piece = resid[rows, c * LANES : (c + 1) * LANES].astype(jnp.float32)
            squares = squares + piece * piece
        sum_row = jnp.sum(jnp.transpose(squares), axis=0, keepdims=True)
        part[0, h : 2 * h, rows] = jnp.broadcast_to(sum_row, (h, count))

    def send_heads(i):
        for off in range(1, n_mp):
            part_copy(off, i).start()

    with jax.named_scope("otherw"):
        other_w("wait")
    for i in range(len(second_ranges)):
        with jax.named_scope("attnw"):
            hid_copy(i).wait()
            for off in range(1, n_mp):
                attn_copy(off, i).wait()
        second_half(i)
        if i > 0:
            head_sums(i - 1)
            send_heads(i - 1)
    with jax.named_scope("heads"):
        head_sums(len(head_ranges) - 1)
        send_heads(len(head_ranges) - 1)

    with jax.named_scope("gap"):
        for copy in small[2:]:
            copy.wait()
        all_slots = seq_s.shape[0]
        slot_lane = lax.broadcasted_iota(jnp.int32, (1, all_slots), 1)
        seq_row = seq_v[...].reshape(1, all_slots)
        token = lax.broadcasted_iota(jnp.int32, (1, block_len), 1).astype(jnp.float32)
        for j in range(slots):
            seq = seq_s[base + j]
            earlier = jnp.where((seq_row == seq) & (slot_lane < base + j), 1.0, 0.0)
            rank = jnp.sum(earlier, axis=1, keepdims=True)
            length = len_s[jnp.maximum(seq, 0)].astype(jnp.float32)
            valid = length - rank * float(block_len)
            live[j : j + 1, :] = jnp.where(token < valid, 1.0, 0.0)

    def own_at(m):
        return m if n_mp == 2 else lax.rem(m + n_mp - mp, n_mp)

    def finish(i):
        rows = block_rows(head_ranges[i])
        for off in range(1, n_mp):
            part_copy(off, i).wait()
        total = part[own_at(0), :, rows]
        for m in range(1, n_mp):
            total = total + part[own_at(m), :, rows]
        scale = lax.rsqrt(total[head_count:] / model_width + norm_epsilon)
        values = total[:head_count] * scale
        for b, j in enumerate(range(*head_ranges[i])):
            block = values[:, b * block_len : (b + 1) * block_len] * live[pl.ds(j, 1), :]
            rewards[j] = block
            sums = jnp.sum(block, axis=1, keepdims=True)
            seq_acc[...] += jnp.where(seq_lane == seq_s[base + j], sums, 0.0)

    with jax.named_scope("fin0"):
        for i in range(len(head_ranges) - 1):
            finish(i)
    def send_body(r, carry):
        low_dest = r * OWN_CAP
        found = jnp.int32(0)
        for j in range(slots):
            d = dest_s[base + j]
            found = jnp.where((d >= low_dest) & (d < low_dest + OWN_CAP), jnp.int32(j), found)
        send_idx[r] = found
        return carry

    with jax.named_scope("sidx"):
        lax.fori_loop(0, n_dp, send_body, 0)
    with jax.named_scope("finl"):
        finish(len(head_ranges) - 1)
    for k in range(n_dp - 1, 0, -1):
        sum_copy(k).start()

    def fill(r, carry):
        send_buf[r] = rewards[send_idx[r]]
        return carry

    lax.fori_loop(0, n_dp, fill, 0, unroll=n_dp <= 16)
    for k in range(n_dp - 1, 0, -1):
        rew_copy(k).start()
    recv_sum[dp] = seq_acc[...]
    recv_rew[dp] = rewards[send_idx[dp]]
    dest_row = dest_v[...].reshape(1, all_slots)
    sources = []
    for q in range(OWN_CAP):
        place = jnp.max(jnp.where(dest_row == dp * OWN_CAP + q, slot_lane, 0))
        sources.append(lax.div(place, slots))
    lengths_row = len_v[...].reshape(1, seq_count).astype(jnp.float32)

    with jax.named_scope("sumw"):
        wait_all(recv_sum, sum_send)
        wait_all(recv_sum, sum_recv)
    totals = recv_sum[0]
    for s in range(1, n_dp):
        totals = totals + recv_sum[s]
    scores = totals[:, :seq_count] / lengths_row
    worst = jnp.min(scores, axis=0, keepdims=True)
    centred = scores - jnp.mean(scores, axis=0, keepdims=True)
    spread = jnp.mean(centred * centred, axis=0, keepdims=True)
    penalty_scale = jnp.mean(spread, axis=1, keepdims=True) + stat_epsilon
    conservative = worst - spread / penalty_scale
    shifted = conservative - jnp.mean(conservative, axis=1, keepdims=True)
    variance = jnp.mean(shifted * shifted, axis=1, keepdims=True)
    adv_buf[...] = jnp.zeros_like(adv_buf)
    adv_buf[0:1, :seq_count] = shifted * lax.rsqrt(variance + stat_epsilon)
    width = adv_buf.shape[1]
    seq_local = adv_out.shape[1]
    turned = pltpu.roll(adv_buf[...], width - dp * seq_local, 1)
    adv_out[...] = turned[0:1, :seq_local]
    with jax.named_scope("reww"):
        wait_all(recv_rew, rew_send)
        wait_all(recv_rew, rew_recv)
    with jax.named_scope("outs"):
        for q in range(OWN_CAP):
            rewards_out[q] = recv_rew[sources[q]]


def store_kernel(rewards_ref, adv_ref, rewards_hbm, adv_hbm, sems):
    copies = [
        pltpu.make_async_copy(rewards_ref, rewards_hbm, sems.at[0]),
        pltpu.make_async_copy(adv_ref, adv_hbm, sems.at[1]),
    ]
    for copy in copies:
        copy.start()
    for copy in copies:
        copy.wait()


def local(n_dp, n_mp, hidden, attn_out, out_proj, norm_gain, reward_proj, block_seq, block_dest, lengths):
    slots, block_len, k_local = attn_out.shape
    n_local = out_proj.shape[1]
    seq_count = lengths.shape[0]
    seq_pad = -(-seq_count // LANES) * LANES
    heads = reward_proj.shape[1]
    groups = split_slots(slots)
    n_first, n_second, n_heads = map(len, groups)
    total_rows = slots * block_len
    f32, bf16 = jnp.float32, jnp.bfloat16
    dma = pltpu.SemaphoreType.DMA
    any_spec = pl.BlockSpec(memory_space=pl.ANY)
    vmem_spec = pl.BlockSpec(memory_space=pltpu.VMEM)
    in_hbm = functools.partial(pltpu.with_memory_space_constraint, memory_space=pltpu.HBM)
    in_vmem = functools.partial(pltpu.with_memory_space_constraint, memory_space=pltpu.VMEM)
    rewards_shape = (OWN_CAP, heads, block_len)
    adv_shape = (1, seq_count // n_dp)
    results = pl.pallas_call(
        functools.partial(kernel, n_dp, n_mp, slots, block_len, seq_count, groups),
        out_shape=(pltpu.VMEM(rewards_shape, f32), pltpu.VMEM(adv_shape, f32)),
        in_specs=[any_spec] * 8,
        out_specs=(vmem_spec, vmem_spec),
        scratch_shapes=[
            pltpu.VMEM((n_mp, total_rows, k_local), bf16),
            pltpu.VMEM((n_mp, k_local, n_local), bf16),
            pltpu.VMEM((total_rows, n_local), bf16),
            pltpu.VMEM((total_rows, n_local), f32),
            pltpu.VMEM((total_rows, n_local), bf16),
            pltpu.VMEM((4 * heads, n_local), bf16),
            pltpu.VMEM((n_mp, 2 * heads, total_rows), f32),
            pltpu.VMEM((slots + (-slots) % 8, block_len), f32),
            pltpu.VMEM((slots, heads, block_len), f32),
            pltpu.VMEM((heads, seq_pad), f32),
            pltpu.VMEM((n_dp, heads, block_len), f32),
            pltpu.VMEM((n_dp, heads, seq_pad), f32),
            pltpu.VMEM((n_dp, heads, block_len), f32),
            pltpu.VMEM((8, seq_pad), f32),
            pltpu.SMEM((n_dp,), jnp.int32),
            pltpu.VMEM(norm_gain.shape, f32),
            pltpu.VMEM((heads, n_local), f32),
            pltpu.SMEM(block_seq.shape, jnp.int32),
            pltpu.SMEM(block_dest.shape, jnp.int32),
            pltpu.SMEM(lengths.shape, jnp.int32),
            pltpu.VMEM(block_seq.shape, jnp.int32),
            pltpu.VMEM(block_dest.shape, jnp.int32),
            pltpu.VMEM(lengths.shape, jnp.int32),
            dma((8,)),
            dma((n_mp, 2)),
            dma((n_first + 1,)),
            dma((n_second,)),
            dma((n_mp - 1, n_second)),
            dma((n_mp - 1, n_second)),
            dma((n_mp - 1, n_heads)),
            dma((n_mp - 1, n_heads)),
            *[dma] * 4,
        ],
        compiler_params=pltpu.CompilerParams(
            collective_id=0, has_side_effects=True, vmem_limit_bytes=40 * 1024 * 1024
        ),
    )(
        in_hbm(hidden.reshape(total_rows, n_local)),
        in_hbm(attn_out.reshape(total_rows, k_local)),
        in_hbm(out_proj),
        in_hbm(norm_gain),
        in_hbm(reward_proj.T),
        in_hbm(block_seq),
        in_hbm(block_dest),
        in_hbm(lengths),
    )
    token_rewards, advantages = pl.pallas_call(
        store_kernel,
        out_shape=(jax.ShapeDtypeStruct(rewards_shape, f32), jax.ShapeDtypeStruct(adv_shape, f32)),
        in_specs=[vmem_spec] * 2,
        out_specs=(any_spec, any_spec),
        scratch_shapes=[dma((2,))],
    )(*map(in_vmem, results))
    return token_rewards, advantages.reshape(seq_count // n_dp)


def solution(mesh):
    return jax.shard_map(
        functools.partial(local, mesh.shape["dp"], mesh.shape["mp"]),
        mesh=mesh,
        in_specs=(
            P("dp", None, "mp"),
            P("dp", None, "mp"),
            P(None, "mp"),
            P("mp"),
            P("mp", None),
            P(),
            P(),
            P(),
        ),
        out_specs=(P("dp", None, None), P("dp")),
        check_vma=False,
    )
```

```python
import functools

import jax
import jax.numpy as jnp
from jax import lax
from jax.experimental import pallas as pl
from jax.experimental.pallas import tpu as pltpu
from jax.sharding import PartitionSpec as P

OWN_CAP = 10

norm_epsilon = 1e-05
stat_epsilon = 1e-06
MESH = pl.DeviceIdType.MESH
LANES = 128


def split_size(slots):
    for size in (5, 4, 3, 2):
        if slots % size == 0:
            return size
    return 1


def partner(index, k, n):
    if n & (n - 1):
        return lax.rem(index + k, n)
    out = index
    bit = 1
    while bit < n:
        if k & bit:
            out = out + bit - 2 * bit * lax.rem(lax.div(index, bit), 2)
        bit *= 2
    return out


def kernel(
    n_dp, n_mp, slots, block_len, seq_count, per_group,
    hidden_hbm, attn_hbm, w_hbm, gain_hbm, reward_hbm, seq_hbm, dest_hbm, len_hbm,
    rewards_out, adv_out,
    attn, w, hidden, acc, resid, heads_w, part, live, rewards, seq_acc, send_buf,
    recv_sum, recv_rew, adv_buf,
    send_idx, gain_ref, reward_ref, seq_s, dest_s, len_s, seq_v, dest_v, len_v, small_sem,
    w_sem, own_sem, hid_sem, attn_send, attn_recv, part_send, part_recv,
    sum_send, sum_recv, rew_send, rew_recv,
):
    dp = lax.axis_index("dp")
    mp = lax.axis_index("mp")
    n_groups = slots // per_group
    rows = per_group * block_len
    k_local = attn_hbm.shape[1]
    n_local = w_hbm.shape[1]
    model_width = w_hbm.shape[0]
    chunk = min(256, n_local)
    n_chunks = n_local // chunk
    head_count = reward_ref.shape[0]
    h = head_count
    base = dp * slots

    barrier = pltpu.get_barrier_semaphore()
    for off in range(1, n_mp):
        pl.semaphore_signal(barrier, inc=1, device_id=(dp, lax.rem(mp + off, n_mp)), device_id_type=MESH)
    across = lax.rem(mp + 1, n_mp) if n_mp == 2 else mp
    for k in range(n_dp - 1, 0, -1):
        pl.semaphore_signal(barrier, inc=1, device_id=(partner(dp, k, n_dp), across), device_id_type=MESH)

    def group_rows(g):
        return pl.ds(pl.multiple_of(g * rows, rows), rows)

    lead_rows, rest_rows = slice(0, rows), slice(rows, slots * block_len)

    k_half = k_local // 2

    def w_copy(off, half):
        start = pl.multiple_of(lax.rem(mp + off, n_mp) * k_local + half * k_half, k_half)
        return pltpu.make_async_copy(
            w_hbm.at[pl.ds(start, k_half)], w.at[off, half * k_half : (half + 1) * k_half], w_sem.at[off, half]
        )

    def lead_copy(half):
        cols = slice(half * k_half, (half + 1) * k_half)
        return pltpu.make_async_copy(attn_hbm.at[lead_rows, cols], attn.at[0, lead_rows, cols], own_sem.at[half])

    def rest_copy():
        return pltpu.make_async_copy(attn_hbm.at[rest_rows], attn.at[0, rest_rows], own_sem.at[2])

    def other_w(action):
        for off in range(1, n_mp):
            for half in range(2):
                getattr(w_copy(off, half), action)()

    def hid_copy():
        return pltpu.make_async_copy(hidden_hbm, hidden, hid_sem)

    def attn_copy(off, g):
        return pltpu.make_async_remote_copy(
            src_ref=attn_hbm.at[group_rows(g)],
            dst_ref=attn.at[n_mp - off, group_rows(g)],
            send_sem=attn_send.at[off - 1, g],
            recv_sem=attn_recv.at[off - 1, g],
            device_id=(dp, lax.rem(mp + off, n_mp)),
            device_id_type=MESH,
        )

    def part_copy(off, g):
        return pltpu.make_async_remote_copy(
            src_ref=part.at[0, g],
            dst_ref=part.at[n_mp - off, g],
            send_sem=part_send.at[off - 1, g],
            recv_sem=part_recv.at[off - 1, g],
            device_id=(dp, lax.rem(mp + off, n_mp)),
            device_id_type=MESH,
        )

    def sum_copy(k):
        return pltpu.make_async_remote_copy(
            src_ref=seq_acc,
            dst_ref=recv_sum.at[dp],
            send_sem=sum_send,
            recv_sem=sum_recv,
            device_id=(partner(dp, k, n_dp), across),
            device_id_type=MESH,
        )

    def rew_copy(k):
        peer = partner(dp, k, n_dp)
        return pltpu.make_async_remote_copy(
            src_ref=send_buf.at[peer],
            dst_ref=recv_rew.at[dp],
            send_sem=rew_send,
            recv_sem=rew_recv,
            device_id=(peer, across),
            device_id_type=MESH,
        )

    def wait_all(ref, sem):
        others = ref.at[0 : n_dp - 1]
        pltpu.make_async_copy(others, others, sem).wait()

    w_copy(0, 0).start()
    lead_copy(0).start()
    small = [
        pltpu.make_async_copy(src, dst, small_sem.at[i])
        for i, (src, dst) in enumerate(
            (
                (gain_hbm, gain_ref),
                (reward_hbm, reward_ref),
                (dest_hbm, dest_s),
                (seq_hbm, seq_s),
                (len_hbm, len_s),
                (seq_hbm, seq_v),
                (dest_hbm, dest_v),
                (len_hbm, len_v),
            )
        )
    ]
    for copy in small:
        copy.start()
    w_copy(0, 1).start(priority=1)
    lead_copy(1).start(priority=1)
    if n_groups > 1:
        rest_copy().start(priority=1)
    with jax.named_scope("smallw"):
        small[0].wait()
        small[1].wait()
    weighted = reward_ref[...] * gain_ref[...].reshape(1, n_local)
    high = weighted.astype(jnp.bfloat16)
    rest = weighted - high.astype(jnp.float32)
    middle = rest.astype(jnp.bfloat16)
    low = (rest - middle.astype(jnp.float32)).astype(jnp.bfloat16)
    heads_w[...] = jnp.concatenate([high, middle, low, jnp.zeros_like(low)], axis=0)
    seq_acc[...] = jnp.zeros_like(seq_acc)

    def lead(half):
        depth = slice(half * k_half, (half + 1) * k_half)
        for c in range(n_chunks):
            cols = slice(c * chunk, (c + 1) * chunk)
            product = jnp.dot(attn[0, lead_rows, depth], w[0, depth, cols], preferred_element_type=jnp.float32)
            acc[lead_rows, cols] = acc[lead_rows, cols] + product if half else product

    def send_attn(i):
        if i < n_groups:
            for off in range(1, n_mp):
                attn_copy(off, i).start()

    with jax.named_scope("sidxw"):
        small[2].wait()
    def send_body(r, carry):
        low_dest = r * OWN_CAP
        found = jnp.int32(0)
        for j in range(slots):
            d = dest_s[base + j]
            found = jnp.where((d >= low_dest) & (d < low_dest + OWN_CAP), jnp.int32(j), found)
        send_idx[r] = found
        return carry

    with jax.named_scope("sidx"):
        lax.fori_loop(0, n_dp, send_body, 0)
    with jax.named_scope("lead0"):
        w_copy(0, 0).wait()
        lead_copy(0).wait()
    lead(0)
    with jax.named_scope("barr"):
        pl.semaphore_wait(barrier, n_mp - 1 + n_dp - 1)
    send_attn(0)
    with jax.named_scope("lead1"):
        w_copy(0, 1).wait()
        lead_copy(1).wait()
    lead(1)
    send_attn(1)
    if n_groups > 1:
        with jax.named_scope("ownw"):
            rest_copy().wait()
    other_w("start")
    hid_copy().start()
    if n_groups > 1:
        for c in range(n_chunks):
            cols = slice(c * chunk, (c + 1) * chunk)
            acc[rest_rows, cols] = jnp.dot(
                attn[0, rest_rows, :], w[0, :, cols], preferred_element_type=jnp.float32
            )
    for g in range(2, n_groups):
        send_attn(g)

    seq_lane = lax.broadcasted_iota(jnp.int32, (head_count, seq_acc.shape[1]), 1)

    def second_half(g, carry):
        with jax.named_scope("attnw"):
            for off in range(1, n_mp):
                attn_copy(off, g).wait_recv()
        squares = jnp.zeros((rows, LANES), jnp.float32)
        for c in range(n_chunks):
            cols = slice(c * chunk, (c + 1) * chunk)
            total = acc[group_rows(g), cols]
            for off in range(1, n_mp):
                total = total + jnp.dot(
                    attn[off, group_rows(g), :], w[off, :, cols], preferred_element_type=jnp.float32
                )
            stored = (hidden[group_rows(g), cols].astype(jnp.float32) + total).astype(jnp.bfloat16)
            resid[:, cols] = stored
            v = stored.astype(jnp.float32)
            for i in range(chunk // LANES):
                piece = v[:, i * LANES : (i + 1) * LANES]
                squares = squares + piece * piece
        out = lax.dot_general(
            heads_w[...], resid[...], (((1,), (1,)), ((), ())), preferred_element_type=jnp.float32
        )
        part[0, g, 0:h, :] = out[0:h] + out[h : 2 * h] + out[2 * h : 3 * h]
        sum_row = jnp.sum(jnp.transpose(squares), axis=0, keepdims=True)
        part[0, g, h : 2 * h, :] = jnp.broadcast_to(sum_row, (h, rows))
        for off in range(1, n_mp):
            part_copy(off, g).start()
        return carry

    with jax.named_scope("otherw"):
        other_w("wait")
        hid_copy().wait()
    lax.fori_loop(0, n_groups, second_half, 0)

    with jax.named_scope("gap"):
        for copy in small[3:]:
            copy.wait()
        all_slots = seq_s.shape[0]
        slot_lane = lax.broadcasted_iota(jnp.int32, (1, all_slots), 1)
        seq_row = seq_v[...].reshape(1, all_slots)
        token = lax.broadcasted_iota(jnp.int32, (1, block_len), 1).astype(jnp.float32)
        for j in range(slots):
            seq = seq_s[base + j]
            earlier = jnp.where((seq_row == seq) & (slot_lane < base + j), 1.0, 0.0)
            rank = jnp.sum(earlier, axis=1, keepdims=True)
            length = len_s[jnp.maximum(seq, 0)].astype(jnp.float32)
            valid = length - rank * float(block_len)
            live[j : j + 1, :] = jnp.where(token < valid, 1.0, 0.0)

    def own_at(m):
        return m if n_mp == 2 else lax.rem(m + n_mp - mp, n_mp)

    def finish(g):
        for off in range(1, n_mp):
            part_copy(off, g).wait_recv()
        total = part[own_at(0), g]
        for m in range(1, n_mp):
            total = total + part[own_at(m), g]
        scale = lax.rsqrt(total[h:] / model_width + norm_epsilon)
        values = total[:h] * scale
        for b in range(per_group):
            j = g * per_group + b
            block = values[:, b * block_len : (b + 1) * block_len] * live[pl.ds(j, 1), :]
            rewards[j] = block
            sums = jnp.sum(block, axis=1, keepdims=True)
            seq_acc[...] += jnp.where(seq_lane == seq_s[base + j], sums, 0.0)

    with jax.named_scope("fin0"):
        for g in range(n_groups - 1):
            finish(g)
    with jax.named_scope("finl"):
        finish(n_groups - 1)
    for k in range(n_dp - 1, 0, -1):
        sum_copy(k).start()

    def fill(r, carry):
        send_buf[r] = rewards[send_idx[r]].astype(send_buf.dtype)
        return carry

    lax.fori_loop(0, n_dp, fill, 0, unroll=n_dp <= 16)
    for k in range(n_dp - 1, 0, -1):
        rew_copy(k).start()
    recv_sum[dp] = seq_acc[...]
    recv_rew[dp] = rewards[send_idx[dp]].astype(recv_rew.dtype)
    dest_row = dest_v[...].reshape(1, all_slots)
    sources = []
    for q in range(OWN_CAP):
        place = jnp.max(jnp.where(dest_row == dp * OWN_CAP + q, slot_lane, 0))
        sources.append(lax.div(place, slots))
    lengths_row = len_v[...].reshape(1, seq_count).astype(jnp.float32)

    with jax.named_scope("sumw"):
        wait_all(recv_sum, sum_recv)
    totals = recv_sum[0]
    for s in range(1, n_dp):
        totals = totals + recv_sum[s]
    scores = totals[:, :seq_count] / lengths_row
    worst = jnp.min(scores, axis=0, keepdims=True)
    centred = scores - jnp.mean(scores, axis=0, keepdims=True)
    spread = jnp.mean(centred * centred, axis=0, keepdims=True)
    spread_mean = jnp.mean(spread, axis=1, keepdims=True)
    worst_mean = jnp.mean(worst, axis=1, keepdims=True)
    penalty_scale = spread_mean + stat_epsilon
    shifted = (worst - spread / penalty_scale) - (worst_mean - spread_mean / penalty_scale)
    variance = jnp.mean(shifted * shifted, axis=1, keepdims=True)
    adv_buf[...] = jnp.zeros_like(adv_buf)
    adv_buf[0:1, :seq_count] = shifted * lax.rsqrt(variance + stat_epsilon)
    width = adv_buf.shape[1]
    seq_local = adv_out.shape[1]
    turned = pltpu.roll(adv_buf[...], width - dp * seq_local, 1)
    adv_out[...] = turned[0:1, :seq_local]
    with jax.named_scope("reww"):
        wait_all(recv_rew, rew_recv)
    with jax.named_scope("outs"):
        for q in range(OWN_CAP):
            rewards_out[q] = recv_rew[sources[q]].astype(jnp.float32)
    with jax.named_scope("sends"):
        for off in range(1, n_mp):
            for g in range(n_groups):
                part_copy(off, g).wait_send()
                attn_copy(off, g).wait_send()
        wait_all(recv_sum, sum_send)
        wait_all(recv_rew, rew_send)


def store_kernel(rewards_ref, adv_ref, rewards_hbm, adv_hbm, sems):
    copies = [
        pltpu.make_async_copy(rewards_ref, rewards_hbm, sems.at[0]),
        pltpu.make_async_copy(adv_ref, adv_hbm, sems.at[1]),
    ]
    for copy in copies:
        copy.start()
    for copy in copies:
        copy.wait()


REW = jnp.bfloat16


def local(n_dp, n_mp, hidden, attn_out, out_proj, norm_gain, reward_proj, block_seq, block_dest, lengths):
    slots, block_len, k_local = attn_out.shape
    n_local = out_proj.shape[1]
    seq_count = lengths.shape[0]
    seq_pad = -(-seq_count // LANES) * LANES
    heads = reward_proj.shape[1]
    per_group = split_size(slots)
    n_groups = slots // per_group
    rows = per_group * block_len
    total_rows = slots * block_len
    f32, bf16 = jnp.float32, jnp.bfloat16
    dma = pltpu.SemaphoreType.DMA
    any_spec = pl.BlockSpec(memory_space=pl.ANY)
    vmem_spec = pl.BlockSpec(memory_space=pltpu.VMEM)
    in_hbm = functools.partial(pltpu.with_memory_space_constraint, memory_space=pltpu.HBM)
    in_vmem = functools.partial(pltpu.with_memory_space_constraint, memory_space=pltpu.VMEM)
    rewards_shape = (OWN_CAP, heads, block_len)
    adv_shape = (1, seq_count // n_dp)
    results = pl.pallas_call(
        functools.partial(kernel, n_dp, n_mp, slots, block_len, seq_count, per_group),
        out_shape=(pltpu.VMEM(rewards_shape, f32), pltpu.VMEM(adv_shape, f32)),
        in_specs=[any_spec] * 8,
        out_specs=(vmem_spec, vmem_spec),
        scratch_shapes=[
            pltpu.VMEM((n_mp, total_rows, k_local), bf16),
            pltpu.VMEM((n_mp, k_local, n_local), bf16),
            pltpu.VMEM((total_rows, n_local), bf16),
            pltpu.VMEM((total_rows, n_local), f32),
            pltpu.VMEM((rows, n_local), bf16),
            pltpu.VMEM((4 * heads, n_local), bf16),
            pltpu.VMEM((n_mp, n_groups, 2 * heads, rows), f32),
            pltpu.VMEM((slots + (-slots) % 8, block_len), f32),
            pltpu.VMEM((slots, heads, block_len), f32),
            pltpu.VMEM((heads, seq_pad), f32),
            pltpu.VMEM((n_dp, heads, block_len), REW),
            pltpu.VMEM((n_dp, heads, seq_pad), f32),
            pltpu.VMEM((n_dp, heads, block_len), REW),
            pltpu.VMEM((8, seq_pad), f32),
            pltpu.SMEM((n_dp,), jnp.int32),
            pltpu.VMEM(norm_gain.shape, f32),
            pltpu.VMEM((heads, n_local), f32),
            pltpu.SMEM(block_seq.shape, jnp.int32),
            pltpu.SMEM(block_dest.shape, jnp.int32),
            pltpu.SMEM(lengths.shape, jnp.int32),
            pltpu.VMEM(block_seq.shape, jnp.int32),
            pltpu.VMEM(block_dest.shape, jnp.int32),
            pltpu.VMEM(lengths.shape, jnp.int32),
            dma((8,)),
            dma((n_mp, 2)),
            dma((3,)),
            dma,
            dma((n_mp - 1, n_groups)),
            dma((n_mp - 1, n_groups)),
            dma((n_mp - 1, n_groups)),
            dma((n_mp - 1, n_groups)),
            *[dma] * 4,
        ],
        compiler_params=pltpu.CompilerParams(
            collective_id=0, has_side_effects=True, vmem_limit_bytes=40 * 1024 * 1024
        ),
    )(
        in_hbm(hidden.reshape(total_rows, n_local)),
        in_hbm(attn_out.reshape(total_rows, k_local)),
        in_hbm(out_proj),
        in_hbm(norm_gain),
        in_hbm(reward_proj.T),
        in_hbm(block_seq),
        in_hbm(block_dest),
        in_hbm(lengths),
    )
    token_rewards, advantages = pl.pallas_call(
        store_kernel,
        out_shape=(jax.ShapeDtypeStruct(rewards_shape, f32), jax.ShapeDtypeStruct(adv_shape, f32)),
        in_specs=[vmem_spec] * 2,
        out_specs=(any_spec, any_spec),
        scratch_shapes=[dma((2,))],
    )(*map(in_vmem, results))
    return token_rewards, advantages.reshape(seq_count // n_dp)


def solution(mesh):
    return jax.shard_map(
        functools.partial(local, mesh.shape["dp"], mesh.shape["mp"]),
        mesh=mesh,
        in_specs=(
            P("dp", None, "mp"),
            P("dp", None, "mp"),
            P(None, "mp"),
            P("mp"),
            P("mp", None),
            P(),
            P(),
            P(),
        ),
        out_specs=(P("dp", None, None), P("dp")),
        check_vma=False,
    )
```

```python
import functools

import jax
import jax.numpy as jnp
from jax import lax
from jax.experimental import pallas as pl
from jax.experimental.pallas import tpu as pltpu
from jax.sharding import PartitionSpec as P

OWN_CAP = 10

norm_epsilon = 1e-05
stat_epsilon = 1e-06
MESH = pl.DeviceIdType.MESH
LANES = 128


def split_size(slots):
    for size in (5, 4, 3, 2):
        if slots % size == 0:
            return size
    return 1


def partner(index, k, n):
    if n & (n - 1):
        return lax.rem(index + k, n)
    out = index
    bit = 1
    while bit < n:
        if k & bit:
            out = out + bit - 2 * bit * lax.rem(lax.div(index, bit), 2)
        bit *= 2
    return out


def kernel(
    n_dp, n_mp, slots, block_len, seq_count, per_group,
    hidden_hbm, attn_hbm, w_hbm, gain_hbm, reward_hbm, seq_hbm, dest_hbm, len_hbm,
    rewards_out, adv_out,
    attn, w, hidden, acc, resid, heads_w, part, live, rewards, seq_acc, sum_row, send_buf,
    recv_sum, recv_rew, adv_buf,
    send_idx, gain_ref, reward_ref, seq_s, len_s, seq_v, dest_v, len_v, small_sem,
    w_sem, own_sem, hid_sem, attn_send, attn_recv, part_send, part_recv,
    sum_send, sum_recv, rew_send, rew_recv,
):
    dp = lax.axis_index("dp")
    mp = lax.axis_index("mp")
    n_groups = slots // per_group
    rows = per_group * block_len
    k_local = attn_hbm.shape[1]
    n_local = w_hbm.shape[1]
    model_width = w_hbm.shape[0]
    chunk = min(256, n_local)
    n_chunks = n_local // chunk
    head_count = reward_ref.shape[0]
    h = head_count
    base = dp * slots

    barrier = pltpu.get_barrier_semaphore()
    for off in range(1, n_mp):
        pl.semaphore_signal(barrier, inc=1, device_id=(dp, lax.rem(mp + off, n_mp)), device_id_type=MESH)
    across = lax.rem(mp + 1, n_mp) if n_mp == 2 else mp
    for k in range(n_dp - 1, 0, -1):
        pl.semaphore_signal(barrier, inc=1, device_id=(partner(dp, k, n_dp), across), device_id_type=MESH)

    def group_rows(g):
        return pl.ds(pl.multiple_of(g * rows, rows), rows)

    lead_rows, rest_rows = slice(0, rows), slice(rows, slots * block_len)

    depths = (slice(0, k_local // LEAD), slice(k_local // LEAD, k_local))

    def w_copy(off, part_at):
        depth = depths[part_at]
        start = pl.multiple_of(lax.rem(mp + off, n_mp) * k_local + depth.start, LANES)
        return pltpu.make_async_copy(
            w_hbm.at[pl.ds(start, depth.stop - depth.start)], w.at[off, depth], w_sem.at[off, part_at]
        )

    def lead_copy(part_at):
        depth = depths[part_at]
        return pltpu.make_async_copy(
            attn_hbm.at[lead_rows, depth], attn.at[0, lead_rows, depth], own_sem.at[part_at]
        )

    def rest_copy():
        return pltpu.make_async_copy(attn_hbm.at[rest_rows], attn.at[0, rest_rows], own_sem.at[2])

    def other_w(action):
        for off in range(1, n_mp):
            for i in range(len(depths)):
                getattr(w_copy(off, i), action)()

    def hid_copy():
        return pltpu.make_async_copy(hidden_hbm, hidden, hid_sem)

    def attn_copy(off, g):
        return pltpu.make_async_remote_copy(
            src_ref=attn_hbm.at[group_rows(g)],
            dst_ref=attn.at[n_mp - off, group_rows(g)],
            send_sem=attn_send.at[off - 1],
            recv_sem=attn_recv.at[off - 1, g],
            device_id=(dp, lax.rem(mp + off, n_mp)),
            device_id_type=MESH,
        )

    def part_copy(off, g):
        return pltpu.make_async_remote_copy(
            src_ref=part.at[0, g],
            dst_ref=part.at[n_mp - off, g],
            send_sem=part_send.at[off - 1],
            recv_sem=part_recv.at[off - 1, g],
            device_id=(dp, lax.rem(mp + off, n_mp)),
            device_id_type=MESH,
        )

    def sum_copy(k):
        return pltpu.make_async_remote_copy(
            src_ref=sum_row,
            dst_ref=recv_sum.at[dp],
            send_sem=sum_send,
            recv_sem=sum_recv,
            device_id=(partner(dp, k, n_dp), across),
            device_id_type=MESH,
        )

    def rew_copy(k):
        peer = partner(dp, k, n_dp)
        return pltpu.make_async_remote_copy(
            src_ref=send_buf.at[peer],
            dst_ref=recv_rew.at[dp],
            send_sem=rew_send,
            recv_sem=rew_recv,
            device_id=(peer, across),
            device_id_type=MESH,
        )

    def wait_all(ref, sem):
        others = ref.at[0 : n_dp - 1]
        pltpu.make_async_copy(others, others, sem).wait()

    w_copy(0, 0).start()
    lead_copy(0).start()
    small = [
        pltpu.make_async_copy(src, dst, small_sem.at[i])
        for i, (src, dst) in enumerate(
            (
                (gain_hbm, gain_ref),
                (reward_hbm, reward_ref),
                (dest_hbm, dest_v),
                (seq_hbm, seq_s),
                (len_hbm, len_s),
                (seq_hbm, seq_v),
                (len_hbm, len_v),
            )
        )
    ]
    for copy in small:
        copy.start()
    w_copy(0, 1).start(priority=1)
    lead_copy(1).start(priority=1)
    if n_groups > 1:
        rest_copy().start(priority=1)
    with jax.named_scope("smallw"):
        small[0].wait()
        small[1].wait()
    weighted = reward_ref[...] * gain_ref[...].reshape(1, n_local)
    high = weighted.astype(jnp.bfloat16)
    rest = weighted - high.astype(jnp.float32)
    middle = rest.astype(jnp.bfloat16)
    low = (rest - middle.astype(jnp.float32)).astype(jnp.bfloat16)
    heads_w[...] = jnp.concatenate([high, middle, low, jnp.zeros_like(low)], axis=0)
    seq_acc[...] = jnp.zeros_like(seq_acc)

    def lead(part_at):
        depth = depths[part_at]
        for c in range(n_chunks):
            cols = slice(c * chunk, (c + 1) * chunk)
            product = jnp.dot(attn[0, lead_rows, depth], w[0, depth, cols], preferred_element_type=jnp.float32)
            acc[lead_rows, cols] = acc[lead_rows, cols] + product if part_at else product

    def send_attn(i):
        if i < n_groups:
            for off in range(1, n_mp):
                attn_copy(off, i).start()

    with jax.named_scope("sidxw"):
        small[2].wait()
    with jax.named_scope("sidx"):
        all_slots = dest_v.shape[0]
        slot_lane = lax.broadcasted_iota(jnp.int32, (1, all_slots), 1)
        dest_row = dest_v[...].reshape(1, all_slots)
        own_dest = jnp.where((slot_lane >= base) & (slot_lane < base + slots), dest_row, -1)
        for r in range(n_dp):
            here = (own_dest >= r * OWN_CAP) & (own_dest < (r + 1) * OWN_CAP)
            send_idx[r] = jnp.max(jnp.where(here, slot_lane - base, 0))
    with jax.named_scope("lead0"):
        w_copy(0, 0).wait()
        lead_copy(0).wait()
    lead(0)
    with jax.named_scope("barr"):
        pl.semaphore_wait(barrier, n_mp - 1 + n_dp - 1)
    send_attn(0)
    with jax.named_scope("lead1"):
        w_copy(0, 1).wait()
        lead_copy(1).wait()
    lead(1)
    send_attn(1)
    if n_groups > 1:
        with jax.named_scope("ownw"):
            rest_copy().wait()
    other_w("start")
    hid_copy().start()
    if n_groups > 1:
        for c in range(n_chunks):
            cols = slice(c * chunk, (c + 1) * chunk)
            acc[rest_rows, cols] = jnp.dot(
                attn[0, rest_rows, :], w[0, :, cols], preferred_element_type=jnp.float32
            )
    for g in range(2, n_groups):
        send_attn(g)

    def second_half(g, carry):
        with jax.named_scope("attnw"):
            for off in range(1, n_mp):
                attn_copy(off, g).wait_recv()
        squares = jnp.zeros((rows, LANES), jnp.float32)
        for c in range(n_chunks):
            cols = slice(c * chunk, (c + 1) * chunk)
            total = acc[group_rows(g), cols]
            for off in range(1, n_mp):
                total = total + jnp.dot(
                    attn[off, group_rows(g), :], w[off, :, cols], preferred_element_type=jnp.float32
                )
            stored = (hidden[group_rows(g), cols].astype(jnp.float32) + total).astype(jnp.bfloat16)
            resid[:, cols] = stored
            v = stored.astype(jnp.float32)
            for i in range(chunk // LANES):
                piece = v[:, i * LANES : (i + 1) * LANES]
                squares = squares + piece * piece
        out = lax.dot_general(
            heads_w[...], resid[...], (((1,), (1,)), ((), ())), preferred_element_type=jnp.float32
        )
        part[0, g, 0:h, :] = out[0:h] + out[h : 2 * h] + out[2 * h : 3 * h]
        square_row = jnp.sum(jnp.transpose(squares), axis=0, keepdims=True)
        part[0, g, h : 2 * h, :] = jnp.broadcast_to(square_row, (h, rows))
        for off in range(1, n_mp):
            part_copy(off, g).start()
        return carry

    with jax.named_scope("otherw"):
        other_w("wait")
        hid_copy().wait()
    lax.fori_loop(0, n_groups, second_half, 0)

    with jax.named_scope("gap"):
        for copy in small[3:]:
            copy.wait()
        seq_row = seq_v[...].reshape(1, all_slots)
        token = lax.broadcasted_iota(jnp.int32, (1, block_len), 1).astype(jnp.float32)
        for j in range(slots):
            seq = seq_s[base + j]
            earlier = jnp.where((seq_row == seq) & (slot_lane < base + j), 1.0, 0.0)
            rank = jnp.sum(earlier, axis=1, keepdims=True)
            length = len_s[jnp.maximum(seq, 0)].astype(jnp.float32)
            valid = length - rank * float(block_len)
            live[j : j + 1, :] = jnp.where(token < valid, 1.0, 0.0)

    span = LANES // head_count
    assert slots <= span
    first_seq = seq_s[base]
    lane = lax.broadcasted_iota(jnp.int32, (head_count, LANES), 1)
    seq_lane = lane - span * lax.broadcasted_iota(jnp.int32, (head_count, LANES), 0)

    def own_at(m):
        return m if n_mp == 2 else lax.rem(m + n_mp - mp, n_mp)

    def finish(g):
        for off in range(1, n_mp):
            part_copy(off, g).wait_recv()
        total = part[own_at(0), g]
        for m in range(1, n_mp):
            total = total + part[own_at(m), g]
        scale = lax.rsqrt(total[h:] / model_width + norm_epsilon)
        values = total[:h] * scale
        for b in range(per_group):
            j = g * per_group + b
            block = values[:, b * block_len : (b + 1) * block_len] * live[pl.ds(j, 1), :]
            rewards[j] = block
            sums = jnp.sum(block, axis=1, keepdims=True)
            seq = seq_s[base + j]
            place = jnp.where(seq < 0, LANES, seq - first_seq)
            seq_acc[...] += jnp.where(seq_lane == place, sums, 0.0)

    with jax.named_scope("fin0"):
        for g in range(n_groups - 1):
            finish(g)
    with jax.named_scope("finl"):
        finish(n_groups - 1)
    sum_row[...] = jnp.sum(seq_acc[...], axis=0, keepdims=True)
    for k in range(n_dp - 1, 0, -1):
        sum_copy(k).start()

    def fill(r, carry):
        send_buf[r] = rewards[send_idx[r]].astype(send_buf.dtype)
        return carry

    lax.fori_loop(0, n_dp, fill, 0, unroll=n_dp <= 16)
    for k in range(n_dp - 1, 0, -1):
        rew_copy(k).start()
    recv_sum[dp] = sum_row[...]
    recv_rew[dp] = rewards[send_idx[dp]].astype(recv_rew.dtype)
    sources = []
    for q in range(OWN_CAP):
        place = jnp.max(jnp.where(dest_row == dp * OWN_CAP + q, slot_lane, 0))
        sources.append(lax.div(place, slots))
    lengths_row = len_v[...].reshape(1, seq_count).astype(jnp.float32)

    with jax.named_scope("sumw"):
        wait_all(recv_sum, sum_recv)
    tiles = [jnp.zeros((head_count, LANES), jnp.float32) for _ in range(0, adv_buf.shape[1], LANES)]
    for s in range(n_dp):
        first = seq_s[s * slots]
        turned = pltpu.roll(jnp.broadcast_to(recv_sum[s], (head_count, LANES)), lax.rem(first, LANES), 1)
        local_at = lax.rem(seq_lane - first + LANES * (len(tiles) + 1), LANES)
        for i in range(len(tiles)):
            mine = local_at < span
            if len(tiles) > 1:
                at = local_at + (first - i * LANES)
                mine = mine & (at >= 0) & (at < LANES)
            tiles[i] = tiles[i] + jnp.where(mine, turned, 0.0)
    head_row = lax.broadcasted_iota(jnp.int32, (head_count, LANES), 0)
    for i, tile in enumerate(tiles):
        straight = tile
        for k in range(1, head_count):
            straight = jnp.where(head_row == k, pltpu.roll(tile, LANES - span * k, 1), straight)
        tiles[i] = straight
    totals = jnp.concatenate(tiles, axis=1) if len(tiles) > 1 else tiles[0]
    scores = totals[:, :seq_count] / lengths_row
    worst = jnp.min(scores, axis=0, keepdims=True)
    centred = scores - jnp.mean(scores, axis=0, keepdims=True)
    spread = jnp.mean(centred * centred, axis=0, keepdims=True)
    spread_mean = jnp.mean(spread, axis=1, keepdims=True)
    worst_mean = jnp.mean(worst, axis=1, keepdims=True)
    penalty_scale = spread_mean + stat_epsilon
    centre = worst_mean - spread_mean / penalty_scale
    shifted = (worst - spread / penalty_scale) - centre
    variance = jnp.mean(shifted * shifted, axis=1, keepdims=True)
    width = adv_buf.shape[1]
    seq_local = adv_out.shape[1]
    adv_buf[...] = jnp.zeros_like(adv_buf)
    adv_buf[0:1, :seq_count] = worst
    adv_buf[1:2, :seq_count] = spread
    turned = pltpu.roll(adv_buf[...], width - dp * seq_local, 1)[:, :seq_local]
    own = (turned[0:1] - turned[1:2] / penalty_scale) - centre
    adv_out[...] = own * lax.rsqrt(variance + stat_epsilon)
    with jax.named_scope("reww"):
        wait_all(recv_rew, rew_recv)
    with jax.named_scope("outs"):
        for q in range(OWN_CAP):
            rewards_out[q] = recv_rew[sources[q]].astype(jnp.float32)
    with jax.named_scope("sends"):
        for off in range(1, n_mp):
            pltpu.make_async_copy(part.at[0], part.at[0], part_send.at[off - 1]).wait()
            pltpu.make_async_copy(attn.at[0], attn.at[0], attn_send.at[off - 1]).wait()
        wait_all(recv_sum, sum_send)
        wait_all(recv_rew, rew_send)


def store_kernel(rewards_ref, adv_ref, rewards_hbm, adv_hbm, sems):
    copies = [
        pltpu.make_async_copy(rewards_ref, rewards_hbm, sems.at[0]),
        pltpu.make_async_copy(adv_ref, adv_hbm, sems.at[1]),
    ]
    for copy in copies:
        copy.start()
    for copy in copies:
        copy.wait()


LEAD = 2
REW = jnp.float32


def local(n_dp, n_mp, hidden, attn_out, out_proj, norm_gain, reward_proj, block_seq, block_dest, lengths):
    slots, block_len, k_local = attn_out.shape
    n_local = out_proj.shape[1]
    seq_count = lengths.shape[0]
    seq_pad = -(-seq_count // LANES) * LANES
    heads = reward_proj.shape[1]
    per_group = split_size(slots)
    n_groups = slots // per_group
    rows = per_group * block_len
    total_rows = slots * block_len
    f32, bf16 = jnp.float32, jnp.bfloat16
    dma = pltpu.SemaphoreType.DMA
    any_spec = pl.BlockSpec(memory_space=pl.ANY)
    vmem_spec = pl.BlockSpec(memory_space=pltpu.VMEM)
    in_hbm = functools.partial(pltpu.with_memory_space_constraint, memory_space=pltpu.HBM)
    in_vmem = functools.partial(pltpu.with_memory_space_constraint, memory_space=pltpu.VMEM)
    rewards_shape = (OWN_CAP, heads, block_len)
    adv_shape = (1, seq_count // n_dp)
    results = pl.pallas_call(
        functools.partial(kernel, n_dp, n_mp, slots, block_len, seq_count, per_group),
        out_shape=(pltpu.VMEM(rewards_shape, f32), pltpu.VMEM(adv_shape, f32)),
        in_specs=[any_spec] * 8,
        out_specs=(vmem_spec, vmem_spec),
        scratch_shapes=[
            pltpu.VMEM((n_mp, total_rows, k_local), bf16),
            pltpu.VMEM((n_mp, k_local, n_local), bf16),
            pltpu.VMEM((total_rows, n_local), bf16),
            pltpu.VMEM((total_rows, n_local), f32),
            pltpu.VMEM((rows, n_local), bf16),
            pltpu.VMEM((4 * heads, n_local), bf16),
            pltpu.VMEM((n_mp, n_groups, 2 * heads, rows), f32),
            pltpu.VMEM((slots + (-slots) % 8, block_len), f32),
            pltpu.VMEM((slots, heads, block_len), f32),
            pltpu.VMEM((heads, LANES), f32),
            pltpu.VMEM((1, LANES), f32),
            pltpu.VMEM((n_dp, heads, block_len), REW),
            pltpu.VMEM((n_dp, 1, LANES), f32),
            pltpu.VMEM((n_dp, heads, block_len), REW),
            pltpu.VMEM((8, seq_pad), f32),
            pltpu.SMEM((n_dp,), jnp.int32),
            pltpu.VMEM(norm_gain.shape, f32),
            pltpu.VMEM((heads, n_local), f32),
            pltpu.SMEM(block_seq.shape, jnp.int32),
            pltpu.SMEM(lengths.shape, jnp.int32),
            pltpu.VMEM(block_seq.shape, jnp.int32),
            pltpu.VMEM(block_dest.shape, jnp.int32),
            pltpu.VMEM(lengths.shape, jnp.int32),
            dma((7,)),
            dma((n_mp, 2)),
            dma((3,)),
            dma,
            dma((n_mp - 1,)),
            dma((n_mp - 1, n_groups)),
            dma((n_mp - 1,)),
            dma((n_mp - 1, n_groups)),
            *[dma] * 4,
        ],
        compiler_params=pltpu.CompilerParams(
            collective_id=0, has_side_effects=True, vmem_limit_bytes=40 * 1024 * 1024
        ),
    )(
        in_hbm(hidden.reshape(total_rows, n_local)),
        in_hbm(attn_out.reshape(total_rows, k_local)),
        in_hbm(out_proj),
        in_hbm(norm_gain),
        in_hbm(reward_proj.T),
        in_hbm(block_seq),
        in_hbm(block_dest),
        in_hbm(lengths),
    )
    token_rewards, advantages = pl.pallas_call(
        store_kernel,
        out_shape=(jax.ShapeDtypeStruct(rewards_shape, f32), jax.ShapeDtypeStruct(adv_shape, f32)),
        in_specs=[vmem_spec] * 2,
        out_specs=(any_spec, any_spec),
        scratch_shapes=[dma((2,))],
    )(*map(in_vmem, results))
    return token_rewards, advantages.reshape(seq_count // n_dp)


def solution(mesh):
    return jax.shard_map(
        functools.partial(local, mesh.shape["dp"], mesh.shape["mp"]),
        mesh=mesh,
        in_specs=(
            P("dp", None, "mp"),
            P("dp", None, "mp"),
            P(None, "mp"),
            P("mp"),
            P("mp", None),
            P(),
            P(),
            P(),
        ),
        out_specs=(P("dp", None, None), P("dp")),
        check_vma=False,
    )
```
